32 devices in a mesh: gx: 2 (over x), gy: 4 (over y, core), gz: 4 (over z).
Axes of the slice: x: 2, y: 2, z: 4, core: 2. Of those that a mesh axis runs over, the one named last changes fastest.
Arguments:
- velocity: float32 [3, 32, 64, 1024], P(None, 'gx', 'gy', 'gz'), may hold values from -24 to 24
- metric: float32 [3, 32, 64, 1024], P(None, 'gx', 'gy', 'gz'), may hold values from 0.5 to 2
Outputs:
- viscosity: float32 [32, 64, 1024], P('gx', 'gy', 'gz')
- coefficient: float32 [32, 64], P('gx', 'gy')
The draws below stay inside these ranges and needn't reach their ends.
All inputs are finite; a program needn't handle non-finite values.
Results may differ from the reference program's by a relative error of at most 0.0003.
Values sent between devices are 32-bit elements; how exact they have to be, the bound alone decides.
A program may use at most 64 MiB of HBM per device.

```python
import math
import jax
import jax.numpy as jnp
from jax import lax

NX = 32
NY = 64
NZ = 1024


def draw_velocity(key, part):
    noise_key = jax.random.fold_in(key, 11)
    amplitude = 1.0 + 2.0 * jnp.arange(NZ, dtype=jnp.float32) / NZ
    random_part = jax.random.truncated_normal(noise_key, -4.0, 4.0, (3, NX, NY, NZ), jnp.float32)
    return random_part * amplitude


def block_scale(stream_key, dims, pieces, smallest, top_value):
    loudness = 1.0
    for dim, shards_of in pieces:
        heights = jax.random.uniform(jax.random.fold_in(jax.random.fold_in(stream_key, 6), dim), (shards_of,), jnp.float32, smallest / len(pieces), top_value / len(pieces))
        loudness = loudness * jnp.repeat(jnp.exp(heights), dims[dim] // shards_of).reshape((-1,) + (1,) * (len(dims) - 1 - dim))
    return loudness


def setup_inputs(seed: int = 0) -> dict:
    keys = jax.random.split(jax.random.key(seed), 3)
    return {
        "velocity": draw_velocity(jax.random.fold_in(keys[2], 71), 0),
        "metric": jnp.clip(jnp.exp(math.log(2.0) - 1.3862944 * jax.random.uniform(keys[1], (3, NX, NY, NZ), jnp.float32) ** block_scale(keys[1], (3, NX, NY, NZ), ((1, 2), (2, 4), (3, 4)), -0.2, 0.2)), 0.5, 2.0),
    }


pair_rows = (0, 1, 2, 0, 0, 1)
pair_cols = (0, 1, 2, 1, 2, 2)
pair_weight = (1.0, 1.0, 1.0, 2.0, 2.0, 2.0)
eps_line = 1e-06
ratio_square = 4.0

def pad_axis(values, axis_pos, periodic):
    length_axis = values.shape[axis_pos]
    if periodic:
        return jnp.concatenate([lax.slice_in_dim(values, length_axis - 1, length_axis, axis=axis_pos), values, lax.slice_in_dim(values, 0, 1, axis=axis_pos)], axis=axis_pos)
    widths = [(0, 0)] * values.ndim
    widths[axis_pos] = (1, 1)
    return jnp.pad(values, widths)

def box_three(padded, axis_pos):
    length_axis = padded.shape[axis_pos]
    lower_side = lax.slice_in_dim(padded, 0, length_axis - 2, axis=axis_pos)
    middle = lax.slice_in_dim(padded, 1, length_axis - 1, axis=axis_pos)
    upper_side = lax.slice_in_dim(padded, 2, length_axis, axis=axis_pos)
    return 0.25 * lower_side + 0.5 * middle + 0.25 * upper_side

def gradient_field(velocity_part, metric):
    columns = []
    for direction in range(3):
        padded = pad_axis(velocity_part, direction + 1, direction == 2)
        length_axis = padded.shape[direction + 1]
        differ = lax.slice_in_dim(padded, 2, length_axis, axis=direction + 1) - lax.slice_in_dim(padded, 0, length_axis - 2, axis=direction + 1)
        columns.append(0.5 * metric[direction] * differ)
    return jnp.stack(columns, axis=1)

def strain_parts(gradients):
    strain = 0.5 * (gradients + jnp.swapaxes(gradients, 0, 1))
    magnitude = jnp.sqrt(2.0 * lax.optimization_barrier(jnp.sum(strain * strain, axis=(0, 1))))
    strain_pairs = jnp.stack([strain[row_index, col_index] for row_index, col_index in zip(pair_rows, pair_cols)])
    return (strain_pairs, magnitude)

def make_fields(velocity_part, strain_pairs, magnitude):
    products = jnp.stack([velocity_part[row_index] * velocity_part[col_index] for row_index, col_index in zip(pair_rows, pair_cols)])
    return jnp.concatenate([velocity_part, products, magnitude[None] * strain_pairs], axis=0)

def germano(filtered, strain_hat, magnitude_hat, delta_sq):
    numerator = jnp.zeros_like(delta_sq)
    denominator = jnp.zeros_like(delta_sq)
    for position in range(6):
        row_index = pair_rows[position]
        col_index = pair_cols[position]
        leonard = filtered[3 + position] - filtered[row_index] * filtered[col_index]
        model_term = 2.0 * delta_sq * (filtered[9 + position] - ratio_square * magnitude_hat * strain_hat[position])
        numerator = numerator + pair_weight[position] * leonard * model_term
        denominator = denominator + pair_weight[position] * model_term * model_term
    return (numerator, denominator)

def reference(velocity, metric):
    delta_sq = (metric[0] * metric[1] * metric[2]) ** (-2.0 / 3.0)
    strain_pairs, magnitude = strain_parts(gradient_field(velocity, metric))
    fields = make_fields(velocity, strain_pairs, magnitude)
    filtered = box_three(pad_axis(fields, 1, False), 1)
    filtered = box_three(pad_axis(filtered, 2, False), 2)
    filtered = box_three(pad_axis(filtered, 3, True), 3)
    strain_hat, magnitude_hat = strain_parts(gradient_field(filtered[0:3], metric))
    numerator, denominator = germano(filtered, strain_hat, magnitude_hat, delta_sq)
    line_num = lax.optimization_barrier(jnp.sum(numerator, axis=2)) / NZ
    line_den = lax.optimization_barrier(jnp.sum(denominator, axis=2)) / NZ
    line_coef = line_num / (line_den + eps_line)
    peak_coef = jnp.max(line_coef)
    coefficient = jnp.minimum(line_coef, 0.5 * peak_coef)
    viscosity = coefficient[:, :, None] * delta_sq * magnitude
    return (viscosity, coefficient)
```

```python
import functools

import jax
import jax.numpy as jnp
from jax import lax
from jax.experimental import pallas as pl
from jax.experimental.pallas import tpu as pltpu
from jax.sharding import PartitionSpec as P

MESH = pl.DeviceIdType.MESH
pairs = ((0, 0), (1, 1), (2, 2), (0, 1), (0, 2), (1, 2))
pair_weight = (1.0, 1.0, 1.0, 2.0, 2.0, 2.0)
eps_line = 1e-06
offsets = [(dx, dy, dz) for dz in (1, -1, 0) for dx in (0, 1, -1) for dy in (0, 1, -1) if (dx, dy, dz) != (0, 0, 0)]


def edge_slots(nx):
    ends = [0, 1, nx - 2, nx - 1]
    order = [(f, x) for f in range(6) for x in ends] + [(f, x) for f in range(6) for x in range(2, nx - 2)]
    return {key: 2 * n for n, key in enumerate(order)}


def kernel(sizes, vel, met, visc, coef_out, V, Gv, G, H, D, Q, PK, R, LS, PS, sem_in, send, recv, lsend, lrecv, psend, precv):
    NX, NY, NZ = sizes
    nx, ny, nz = vel.shape[1:]
    yr, zr = ny + 8, nz + 128
    slots = edge_slots(nx)
    lanes_packed = PK.shape[2]
    ix, iy, iz = lax.axis_index("gx"), lax.axis_index("gy"), lax.axis_index("gz")

    load_v = pltpu.make_async_copy(vel, V.at[0:3, 2 : 2 + nx, 0:ny, 0:nz], sem_in.at[0])
    load_m = pltpu.make_async_copy(met, V.at[3:6, 2 : 2 + nx, 0:ny, 0:nz], sem_in.at[1])
    load_v.start()
    load_m.start()

    def exists(d):
        ok = None
        for delta, i, n in ((d[0], ix, NX), (d[1], iy, NY)):
            if delta:
                c = (i + delta >= 0) & (i + delta < n)
                ok = c if ok is None else ok & c
        return ok

    def when(cond, fn):
        if cond is None:
            fn()
        else:
            pl.when(cond)(fn)

    def dev(d):
        return (ix + d[0], iy + d[1], lax.rem(iz + d[2] + NZ, NZ))

    zplane = jnp.zeros((yr, zr), jnp.float32)
    for f in range(6):
        for xi in (0, 1, nx + 2, nx + 3):
            V[f, xi] = zplane
        def clear(x, _, f=f):
            V[f, x, ny:yr, :] = zplane[0:8]
            return 0
        lax.fori_loop(2, 2 + nx, clear, 0)
    for s in range(2):
        for dx in range(3):
            for dy in range(3):
                R[s, dx, dy] = jnp.zeros((ny, lanes_packed), jnp.float32)

    barrier = pltpu.get_barrier_semaphore()
    expected = jnp.int32(0)
    for d in offsets:
        ok = exists(d)
        def sig(d=d):
            pl.semaphore_signal(barrier, inc=1, device_id=dev(d), device_id_type=MESH)
        when(ok, sig)
        expected = expected + (1 if ok is None else ok.astype(jnp.int32))
    for o in range(1, NZ):
        pl.semaphore_signal(barrier, inc=1, device_id=(ix, iy, lax.rem(iz + o, NZ)), device_id_type=MESH)
    plane_peers = [(a, b) for a in range(NX) for b in range(NY) if (a, b) != (0, 0)]
    for a, b in plane_peers:
        pl.semaphore_signal(barrier, inc=1, device_id=(lax.rem(ix + a, NX), lax.rem(iy + b, NY), iz), device_id_type=MESH)
    expected = expected + (NZ - 1 + len(plane_peers))

    load_v.wait()
    load_m.wait()

    lane = lax.broadcasted_iota(jnp.int32, (ny, 128), 1)
    half = lane // 2
    acc = [[jnp.zeros((ny, 128), jnp.float32) for _ in range(lanes_packed // 128)] for _ in range(2)]
    for (f, x), p in slots.items():
        t, l = divmod(p, 128)
        here = half == l // 2
        hi = V[f, x + 2, 0:ny, nz - 128 : nz]
        lo = V[f, x + 2, 0:ny, 0:128]
        s_hi, s_lo = (l - 126) % 128, l
        acc[0][t] = jnp.where(here, pltpu.roll(hi, s_hi, 1) if s_hi else hi, acc[0][t])
        acc[1][t] = jnp.where(here, pltpu.roll(lo, s_lo, 1) if s_lo else lo, acc[1][t])
    for s in range(2):
        for t in range(lanes_packed // 128):
            PK[s, :, 128 * t : 128 * t + 128] = acc[s][t]

    pl.semaphore_wait(barrier, expected)

    def span_x(dx, metric):
        if dx == 0:
            return (2, 2, nx)
        if dx == 1:
            return (nx + 1, 1, 1) if metric else (nx, 0, 2)
        return (2, nx + 2, 1) if metric else (2, nx + 2, 2)

    def span_y(dy, metric):
        if dy == 0:
            return (0, 0, ny)
        if dy == 1:
            return (ny - 1, ny + 7, 1) if metric else (ny - 2, ny + 6, 2)
        return (0, ny, 1) if metric else (0, ny, 2)

    def copies(n, d):
        dx, dy, dz = d
        out = []
        if dz:
            s = 0 if dz == 1 else 1
            r0, rn = (0, ny) if dy == 0 else ((ny - 8, 8) if dy == 1 else (0, 8))
            ln = lanes_packed if dx == 0 else 128
            out.append((PK.at[s, r0 : r0 + rn, 0:ln], R.at[s, dx + 1, dy + 1, r0 : r0 + rn, 0:ln], 2 * n))
        else:
            for k in range(2):
                xs, xd, xn = span_x(dx, k == 1)
                ys, yd, yn = span_y(dy, k == 1)
                f0 = 3 * k
                out.append((
                    V.at[f0 : f0 + 3, xs : xs + xn, ys : ys + yn, 0:nz],
                    V.at[f0 : f0 + 3, xd : xd + xn, yd : yd + yn, 0:nz],
                    2 * n + k,
                ))
        return [
            pltpu.make_async_remote_copy(src_ref=a, dst_ref=b, send_sem=send.at[j], recv_sem=recv.at[j], device_id=dev(d), device_id_type=MESH)
            for a, b, j in out
        ]

    for n, d in enumerate(offsets):
        def go(n=n, d=d):
            for c in copies(n, d):
                c.start()
        when(exists(d), go)
    for n, d in enumerate(offsets):
        def land(n=n, d=d):
            for c in copies(n, d):
                c.wait_recv()
        when(exists((-d[0], -d[1], -d[2])), land)
    for n, d in enumerate(offsets):
        def left(n=n, d=d):
            for c in copies(n, d):
                c.wait_send()
        when(exists(d), left)

    lane_r = lax.broadcasted_iota(jnp.int32, (yr, 128), 1)
    low_rows = lax.broadcasted_iota(jnp.int32, (8, 128), 0) < 4
    def packed(s, dx, t):
        cut = slice(128 * t, 128 * t + 128)
        edge = jnp.where(low_rows, R[s, dx, 0, 0:8, cut], R[s, dx, 2, ny - 8 : ny, cut])
        return jnp.concatenate([R[s, dx, 1, :, cut], edge], axis=0)
    tiles = {}
    for f in range(6):
        for xi in range(nx + 4):
            if f >= 3 and xi in (0, nx + 3):
                continue
            if xi < 2:
                dx, x = 2, nx - 2 + xi
            elif xi >= nx + 2:
                dx, x = 0, xi - nx - 2
            else:
                dx, x = 1, xi - 2
            t, l = divmod(slots[(f, x)], 128)
            for s in range(2):
                if (s, dx, t) not in tiles:
                    tiles[(s, dx, t)] = packed(s, dx, t)
            a = pltpu.roll(tiles[(0, dx, t)], (126 - l) % 128, 1) if l != 126 else tiles[(0, dx, t)]
            b = pltpu.roll(tiles[(1, dx, t)], (128 - l) % 128, 1) if l else tiles[(1, dx, t)]
            V[f, xi, :, nz:zr] = jnp.where(lane_r < 64, b, a)

    def up(a, axis):
        return pltpu.roll(a, a.shape[axis] - 1, axis)

    def down(a, axis):
        return pltpu.roll(a, 1, axis)

    def smooth(a, axis):
        t = a + down(a, axis)
        return t + up(t, axis)

    def velocity_plane(x, _):
        for c in range(3):
            Gv[c, x] = smooth(smooth(V[c, x], 0), 1)
        return 0

    lax.fori_loop(0, nx + 4, velocity_plane, 0)

    def strains(load, m, x):
        d = [[None] * 3 for _ in range(3)]
        for i in range(3):
            here = load(i, x)
            d[i][0] = m[0] * (load(i, x + 1) - load(i, x - 1))
            d[i][1] = m[1] * (up(here, 0) - down(here, 0))
            d[i][2] = m[2] * (up(here, 1) - down(here, 1))
        e = [d[a][b] if a == b else 0.5 * (d[a][b] + d[b][a]) for a, b in pairs]
        square = (e[0] * e[0] + e[1] * e[1] + e[2] * e[2]) + 2.0 * (e[3] * e[3] + e[4] * e[4] + e[5] * e[5])
        return e, jnp.sqrt(0.5 * square)

    def field_plane(x, _):
        m = [V[3 + c, x] for c in range(3)]
        e, mag = strains(lambda i, p: V[i, p], m, x)
        p = m[0][0:ny, 0:nz] * m[1][0:ny, 0:nz] * m[2][0:ny, 0:nz]
        dq = jnp.exp((-2.0 / 3.0) * jnp.log(p))
        Q[x] = dq
        D[x] = dq * mag[0:ny, 0:nz]
        for k, (a, b) in enumerate(pairs):
            G[k, x] = smooth(smooth(V[a, x] * V[b, x], 0)[0:ny], 1)[:, 0:nz]
            G[6 + k, x] = smooth(smooth(mag * e[k], 0)[0:ny], 1)[:, 0:nz]
        return 0

    lax.fori_loop(1, nx + 3, field_plane, 0)

    row = lax.broadcasted_iota(jnp.int32, (yr, zr), 0)
    has_lo = jnp.where(iy > 0, 1.0, 0.0)
    has_hi = jnp.where(iy < NY - 1, 1.0, 0.0)
    row_scale = jnp.where(row < ny, 1.0, jnp.where(row == ny, has_hi, has_lo)) * (1.0 / 64.0)

    def hat_plane(x, _):
        inside = jnp.where((x == 1) & (ix == 0), 0.0, jnp.where((x == nx + 2) & (ix == NX - 1), 0.0, 1.0))
        for c in range(3):
            mid = Gv[c, x]
            H[c, x] = (Gv[c, x - 1] + Gv[c, x + 1] + (mid + mid)) * (row_scale * inside)
        return 0

    lax.fori_loop(1, nx + 3, hat_plane, 0)

    lane_s = lax.broadcasted_iota(jnp.int32, (ny, 128), 1)

    def line_plane(x, sums):
        d = [[None] * 3 for _ in range(3)]
        hat = []
        for i in range(3):
            here = H[i, x]
            core = here[0:ny]
            hat.append(core[:, 0:nz])
            d[i][0] = V[3, x, 0:ny, 0:nz] * (H[i, x + 1, 0:ny, 0:nz] - H[i, x - 1, 0:ny, 0:nz])
            d[i][1] = V[4, x, 0:ny, 0:nz] * (up(here, 0) - down(here, 0))[0:ny, 0:nz]
            d[i][2] = V[5, x, 0:ny, 0:nz] * (up(core, 1) - down(core, 1))[:, 0:nz]
        e = [d[a][b] if a == b else 0.5 * (d[a][b] + d[b][a]) for a, b in pairs]
        square = (e[0] * e[0] + e[1] * e[1] + e[2] * e[2]) + 2.0 * (e[3] * e[3] + e[4] * e[4] + e[5] * e[5])
        mag2 = 2.0 * jnp.sqrt(0.5 * square)
        num = den = 0.0
        for k, (a, b) in enumerate(pairs):
            vv, ms = G[k, x], G[6 + k, x]
            vv = (G[k, x - 1] + G[k, x + 1] + (vv + vv)) * (1.0 / 64.0)
            ms = (G[6 + k, x - 1] + G[6 + k, x + 1] + (ms + ms)) * (1.0 / 128.0)
            leonard = vv - hat[a] * hat[b]
            model = ms - mag2 * e[k]
            n, m2 = leonard * model, model * model
            if pair_weight[k] != 1.0:
                n, m2 = pair_weight[k] * n, pair_weight[k] * m2
            num, den = num + n, den + m2
        dq2 = 2.0 * Q[x]
        num = num * dq2
        den = den * (dq2 * dq2)
        num = jnp.sum(num, axis=1, keepdims=True)
        den = jnp.sum(den, axis=1, keepdims=True)
        sums = jnp.where(lane_s == x - 2, num, sums)
        return jnp.where(lane_s == x + 62, den, sums)

    sums = lax.fori_loop(2, nx + 2, line_plane, jnp.zeros((ny, 128), jnp.float32))

    LS[iz] = sums
    def line_copy(o):
        return pltpu.make_async_remote_copy(
            src_ref=LS.at[iz], dst_ref=LS.at[iz], send_sem=lsend.at[o - 1], recv_sem=lrecv.at[o - 1],
            device_id=(ix, iy, lax.rem(iz + o, NZ)), device_id_type=MESH)
    def line_landing(o):
        src = lax.rem(iz - o + NZ, NZ)
        return pltpu.make_async_remote_copy(
            src_ref=LS.at[src], dst_ref=LS.at[src], send_sem=lsend.at[o - 1], recv_sem=lrecv.at[o - 1],
            device_id=(ix, iy, lax.rem(iz + o, NZ)), device_id_type=MESH)
    for o in range(1, NZ):
        line_copy(o).start()
    for o in range(1, NZ):
        line_landing(o).wait_recv()
    total = LS[0]
    for o in range(1, NZ):
        total = total + LS[o]
    cells = float(nz * NZ)
    line_num = total / cells
    line_den = pltpu.roll(total, 64, 1) / cells
    coef = line_num / (line_den + eps_line)
    here_max = jnp.max(jnp.where(lane_s < nx, coef, -jnp.inf), axis=(0, 1), keepdims=True)
    me = ix * NY + iy
    PS[me] = jnp.broadcast_to(here_max, (8, 128))
    def peak_copy(j, a, b, landing):
        tx, ty = lax.rem(ix + a, NX), lax.rem(iy + b, NY)
        slot = me
        if landing:
            slot = lax.rem(ix - a + NX, NX) * NY + lax.rem(iy - b + NY, NY)
        return pltpu.make_async_remote_copy(
            src_ref=PS.at[slot], dst_ref=PS.at[slot], send_sem=psend.at[j], recv_sem=precv.at[j],
            device_id=(tx, ty, iz), device_id_type=MESH)
    for j, (a, b) in enumerate(plane_peers):
        peak_copy(j, a, b, False).start()
    for o in range(1, NZ):
        line_copy(o).wait_send()
    for j, (a, b) in enumerate(plane_peers):
        peak_copy(j, a, b, True).wait_recv()
    peak = PS[0]
    for j in range(1, NX * NY):
        peak = jnp.maximum(peak, PS[j])
    coef = jnp.minimum(coef, 0.5 * peak[0:1, :])
    for x in range(nx):
        column = jnp.sum(jnp.where(lane_s == x, coef, 0.0), axis=1, keepdims=True)
        visc[x] = D[x + 2] * column
    coef_out[...] = coef
    for j, (a, b) in enumerate(plane_peers):
        peak_copy(j, a, b, False).wait_send()


def per_device(sizes, velocity, metric):
    nx, ny, nz = velocity.shape[1:]
    NX, NY, NZ = sizes
    yr, zr = ny + 8, nz + 128
    packed = -(-12 * nx // 128) * 128
    f32 = jnp.float32
    visc, coef = pl.pallas_call(
        functools.partial(kernel, sizes),
        out_shape=(jax.ShapeDtypeStruct((nx, ny, nz), f32), jax.ShapeDtypeStruct((ny, 128), f32)),
        in_specs=[pl.BlockSpec(memory_space=pl.ANY)] * 2,
        out_specs=(pl.BlockSpec(memory_space=pltpu.VMEM),) * 2,
        scratch_shapes=[
            pltpu.VMEM((6, nx + 4, yr, zr), f32),
            pltpu.VMEM((3, nx + 4, yr, zr), f32),
            pltpu.VMEM((12, nx + 4, ny, nz), f32),
            pltpu.VMEM((3, nx + 4, yr, zr), f32),
            pltpu.VMEM((nx + 4, ny, nz), f32),
            pltpu.VMEM((nx + 4, ny, nz), f32),
            pltpu.VMEM((2, ny, packed), f32),
            pltpu.VMEM((2, 3, 3, ny, packed), f32),
            pltpu.VMEM((NZ, ny, 128), f32),
            pltpu.VMEM((NX * NY, 8, 128), f32),
            pltpu.SemaphoreType.DMA((2,)),
            pltpu.SemaphoreType.DMA((2 * len(offsets),)),
            pltpu.SemaphoreType.DMA((2 * len(offsets),)),
            pltpu.SemaphoreType.DMA((NZ,)),
            pltpu.SemaphoreType.DMA((NZ,)),
            pltpu.SemaphoreType.DMA((NX * NY,)),
            pltpu.SemaphoreType.DMA((NX * NY,)),
        ],
        compiler_params=pltpu.CompilerParams(collective_id=0, has_side_effects=True, vmem_limit_bytes=48 * 1024 * 1024),
    )(velocity, metric)
    return visc, coef[:, :nx].T


def solution(mesh):
    sizes = (mesh.shape["gx"], mesh.shape["gy"], mesh.shape["gz"])
    return jax.shard_map(
        functools.partial(per_device, sizes),
        mesh=mesh,
        in_specs=(P(None, "gx", "gy", "gz"), P(None, "gx", "gy", "gz")),
        out_specs=(P("gx", "gy", "gz"), P("gx", "gy")),
        check_vma=False,
    )
```

```python
import functools

import jax
import jax.numpy as jnp
from jax import lax
from jax.experimental import pallas as pl
from jax.experimental.pallas import tpu as pltpu
from jax.sharding import PartitionSpec as P

MESH = pl.DeviceIdType.MESH
pairs = ((0, 0), (1, 1), (2, 2), (0, 1), (0, 2), (1, 2))
pair_weight = (1.0, 1.0, 1.0, 2.0, 2.0, 2.0)
eps_line = 1e-06
offsets = [(dx, dy, dz) for dz in (1, -1, 0) for dx in (0, 1, -1) for dy in (0, 1, -1) if (dx, dy, dz) != (0, 0, 0)]


def edge_slots(nx):
    ends = [0, 1, nx - 2, nx - 1]
    order = [(f, x) for f in range(6) for x in ends] + [(f, x) for f in range(6) for x in range(2, nx - 2)]
    return {key: 2 * n for n, key in enumerate(order)}


def kernel(sizes, vel, met, D, coef_out, V, Gv, G, H, Q, PK, R, LS, PS, sem_in, send, recv, lsend, lrecv, psend, precv):
    NX, NY, NZ = sizes
    nx, ny, nz = vel.shape[1:]
    yr, zr = ny + 8, nz + 128
    slots = edge_slots(nx)
    lanes_packed = PK.shape[2]
    ix, iy, iz = lax.axis_index("gx"), lax.axis_index("gy"), lax.axis_index("gz")

    load_v = pltpu.make_async_copy(vel, V.at[0:3, 2 : 2 + nx, 0:ny, 0:nz], sem_in.at[0])
    load_m = pltpu.make_async_copy(met, V.at[3:6, 2 : 2 + nx, 0:ny, 0:nz], sem_in.at[1])
    load_v.start()
    load_m.start()

    def exists(d):
        ok = None
        for delta, i, n in ((d[0], ix, NX), (d[1], iy, NY)):
            if delta:
                c = (i + delta >= 0) & (i + delta < n)
                ok = c if ok is None else ok & c
        return ok

    def when(cond, fn):
        if cond is None:
            fn()
        else:
            pl.when(cond)(fn)

    def dev(d):
        return (ix + d[0], iy + d[1], lax.rem(iz + d[2] + NZ, NZ))

    zplane = jnp.zeros((yr, zr), jnp.float32)
    for f in range(6):
        for xi in (0, 1, nx + 2, nx + 3):
            V[f, xi] = zplane
        def clear(x, _, f=f):
            V[f, x, ny:yr, :] = zplane[0:8]
            return 0
        lax.fori_loop(2, 2 + nx, clear, 0)
    for s in range(2):
        for dx in range(3):
            for dy in range(3):
                R[s, dx, dy] = jnp.zeros((ny, lanes_packed), jnp.float32)

    barrier = pltpu.get_barrier_semaphore()
    expected = jnp.int32(0)
    for d in offsets:
        ok = exists(d)
        def sig(d=d):
            pl.semaphore_signal(barrier, inc=1, device_id=dev(d), device_id_type=MESH)
        when(ok, sig)
        expected = expected + (1 if ok is None else ok.astype(jnp.int32))
    for o in range(1, NZ):
        pl.semaphore_signal(barrier, inc=1, device_id=(ix, iy, lax.rem(iz + o, NZ)), device_id_type=MESH)
    plane_peers = [(a, b) for a in range(NX) for b in range(NY) if (a, b) != (0, 0)]
    for a, b in plane_peers:
        pl.semaphore_signal(barrier, inc=1, device_id=(lax.rem(ix + a, NX), lax.rem(iy + b, NY), iz), device_id_type=MESH)
    expected = expected + (NZ - 1 + len(plane_peers))

    load_v.wait()
    load_m.wait()

    lane = lax.broadcasted_iota(jnp.int32, (ny, 128), 1)
    half = lane // 2
    acc = [[jnp.zeros((ny, 128), jnp.float32) for _ in range(lanes_packed // 128)] for _ in range(2)]
    for (f, x), p in slots.items():
        t, l = divmod(p, 128)
        here = half == l // 2
        hi = V[f, x + 2, 0:ny, nz - 128 : nz]
        lo = V[f, x + 2, 0:ny, 0:128]
        s_hi, s_lo = (l - 126) % 128, l
        acc[0][t] = jnp.where(here, pltpu.roll(hi, s_hi, 1) if s_hi else hi, acc[0][t])
        acc[1][t] = jnp.where(here, pltpu.roll(lo, s_lo, 1) if s_lo else lo, acc[1][t])
    for s in range(2):
        for t in range(lanes_packed // 128):
            PK[s, :, 128 * t : 128 * t + 128] = acc[s][t]

    pl.semaphore_wait(barrier, expected)

    def span_x(dx, metric):
        if dx == 0:
            return (2, 2, nx)
        if dx == 1:
            return (nx + 1, 1, 1) if metric else (nx, 0, 2)
        return (2, nx + 2, 1) if metric else (2, nx + 2, 2)

    def span_y(dy, metric):
        if dy == 0:
            return (0, 0, ny)
        if dy == 1:
            return (ny - 1, ny + 7, 1) if metric else (ny - 2, ny + 6, 2)
        return (0, ny, 1) if metric else (0, ny, 2)

    def copies(n, d):
        dx, dy, dz = d
        out = []
        if dz:
            s = 0 if dz == 1 else 1
            r0, rn = (0, ny) if dy == 0 else ((ny - 8, 8) if dy == 1 else (0, 8))
            ln = lanes_packed if dx == 0 else 128
            out.append((PK.at[s, r0 : r0 + rn, 0:ln], R.at[s, dx + 1, dy + 1, r0 : r0 + rn, 0:ln], 2 * n))
        else:
            for k in range(2):
                xs, xd, xn = span_x(dx, k == 1)
                ys, yd, yn = span_y(dy, k == 1)
                f0 = 3 * k
                out.append((
                    V.at[f0 : f0 + 3, xs : xs + xn, ys : ys + yn, 0:nz],
                    V.at[f0 : f0 + 3, xd : xd + xn, yd : yd + yn, 0:nz],
                    2 * n + k,
                ))
        return [
            pltpu.make_async_remote_copy(src_ref=a, dst_ref=b, send_sem=send.at[j], recv_sem=recv.at[j], device_id=dev(d), device_id_type=MESH)
            for a, b, j in out
        ]

    for n, d in enumerate(offsets):
        def go(n=n, d=d):
            for c in copies(n, d):
                c.start()
        when(exists(d), go)
    def land(wanted):
        for n, d in enumerate(offsets):
            if wanted(d):
                def arrive(n=n, d=d):
                    for c in copies(n, d):
                        c.wait_recv()
                when(exists((-d[0], -d[1], -d[2])), arrive)

    land(lambda d: d[0] == 0 and d[2] != 0)

    lane_r = lax.broadcasted_iota(jnp.int32, (yr, 128), 1)
    low_rows = lax.broadcasted_iota(jnp.int32, (8, 128), 0) < 4
    def packed(s, dx, t):
        cut = slice(128 * t, 128 * t + 128)
        edge = jnp.where(low_rows, R[s, dx, 0, 0:8, cut], R[s, dx, 2, ny - 8 : ny, cut])
        return jnp.concatenate([R[s, dx, 1, :, cut], edge], axis=0)
    tiles = {}
    def fill_span(f, planes):
        for xi in planes:
            if f >= 3 and xi in (0, nx + 3):
                continue
            if xi < 2:
                dx, x = 2, nx - 2 + xi
            elif xi >= nx + 2:
                dx, x = 0, xi - nx - 2
            else:
                dx, x = 1, xi - 2
            t, l = divmod(slots[(f, x)], 128)
            for s in range(2):
                if (s, dx, t) not in tiles:
                    tiles[(s, dx, t)] = packed(s, dx, t)
            a = pltpu.roll(tiles[(0, dx, t)], (126 - l) % 128, 1) if l != 126 else tiles[(0, dx, t)]
            b = pltpu.roll(tiles[(1, dx, t)], (128 - l) % 128, 1) if l else tiles[(1, dx, t)]
            V[f, xi, :, nz:zr] = jnp.where(lane_r < 64, b, a)

    for f in range(6):
        fill_span(f, range(2, nx + 2))
    land(lambda d: d[0] == 0 and d[2] == 0)

    def up(a, axis):
        return pltpu.roll(a, a.shape[axis] - 1, axis)

    def down(a, axis):
        return pltpu.roll(a, 1, axis)

    def smooth(a, axis):
        if axis == 1:
            return (a + a) + (up(a, 1) + down(a, 1))
        t = a + down(a, axis)
        return t + up(t, axis)

    def velocity_plane(x, _):
        for c in range(3):
            Gv[c, x] = smooth(smooth(V[c, x], 0), 1)
        return 0


    def strains(load, m, x):
        d = [[None] * 3 for _ in range(3)]
        for i in range(3):
            here = load(i, x)
            d[i][0] = m[0] * (load(i, x + 1) - load(i, x - 1))
            d[i][1] = m[1] * (up(here, 0) - down(here, 0))
            d[i][2] = m[2] * (up(here, 1) - down(here, 1))
        e = [d[a][b] if a == b else 0.5 * (d[a][b] + d[b][a]) for a, b in pairs]
        square = (e[0] * e[0] + e[1] * e[1] + e[2] * e[2]) + 2.0 * (e[3] * e[3] + e[4] * e[4] + e[5] * e[5])
        return e, jnp.sqrt(0.5 * square)

    def field_plane(x, _):
        m = [V[3 + c, x] for c in range(3)]
        e, mag = strains(lambda i, p: V[i, p], m, x)
        p = m[0][0:ny, 0:nz] * m[1][0:ny, 0:nz] * m[2][0:ny, 0:nz]
        dq = jnp.exp((-2.0 / 3.0) * jnp.log(p))
        Q[x] = dq
        D[jnp.clip(x - 2, 0, nx - 1)] = dq * mag[0:ny, 0:nz]
        for k, (a, b) in enumerate(pairs):
            G[k, x] = smooth(smooth(V[a, x] * V[b, x], 0)[0:ny], 1)[:, 0:nz]
            G[6 + k, x] = smooth(smooth(mag * e[k], 0)[0:ny], 1)[:, 0:nz]
        return 0

    lax.fori_loop(2, nx + 2, velocity_plane, 0, unroll=4)
    lax.fori_loop(3, nx + 1, field_plane, 0)
    land(lambda d: d[0] != 0)
    for f in range(6):
        fill_span(f, (0, 1, nx + 2, nx + 3))
    lax.fori_loop(0, 4, lambda i, c: velocity_plane(jnp.where(i < 2, i, nx + i), c), 0)
    lax.fori_loop(0, 4, lambda i, c: field_plane(jnp.where(i < 2, i + 1, nx + 4 - i), c), 0)

    row = lax.broadcasted_iota(jnp.int32, (yr, zr), 0)
    has_lo = jnp.where(iy > 0, 1.0, 0.0)
    has_hi = jnp.where(iy < NY - 1, 1.0, 0.0)
    row_scale = jnp.where(row < ny, 1.0, jnp.where(row == ny, has_hi, has_lo)) * (1.0 / 64.0)

    def hat_plane(x, _):
        inside = jnp.where((x == 1) & (ix == 0), 0.0, jnp.where((x == nx + 2) & (ix == NX - 1), 0.0, 1.0))
        for c in range(3):
            mid = Gv[c, x]
            H[c, x] = (Gv[c, x - 1] + Gv[c, x + 1] + (mid + mid)) * (row_scale * inside)
        return 0

    lax.fori_loop(1, nx + 3, hat_plane, 0)

    lane_s = lax.broadcasted_iota(jnp.int32, (ny, 128), 1)

    def line_plane(x, sums):
        d = [[None] * 3 for _ in range(3)]
        hat = []
        for i in range(3):
            here = H[i, x]
            core = here[0:ny]
            hat.append(core[:, 0:nz])
            d[i][0] = V[3, x, 0:ny, 0:nz] * (H[i, x + 1, 0:ny, 0:nz] - H[i, x - 1, 0:ny, 0:nz])
            d[i][1] = V[4, x, 0:ny, 0:nz] * (up(here, 0) - down(here, 0))[0:ny, 0:nz]
            d[i][2] = V[5, x, 0:ny, 0:nz] * (up(core, 1) - down(core, 1))[:, 0:nz]
        e = [d[a][b] if a == b else 0.5 * (d[a][b] + d[b][a]) for a, b in pairs]
        square = (e[0] * e[0] + e[1] * e[1] + e[2] * e[2]) + 2.0 * (e[3] * e[3] + e[4] * e[4] + e[5] * e[5])
        mag2 = 2.0 * jnp.sqrt(0.5 * square)
        num = den = 0.0
        for k, (a, b) in enumerate(pairs):
            vv, ms = G[k, x], G[6 + k, x]
            vv = (G[k, x - 1] + G[k, x + 1] + (vv + vv)) * (1.0 / 64.0)
            ms = (G[6 + k, x - 1] + G[6 + k, x + 1] + (ms + ms)) * (1.0 / 128.0)
            leonard = vv - hat[a] * hat[b]
            model = ms - mag2 * e[k]
            n, m2 = leonard * model, model * model
            if pair_weight[k] != 1.0:
                n, m2 = pair_weight[k] * n, pair_weight[k] * m2
            num, den = num + n, den + m2
        dq2 = 2.0 * Q[x]
        num = num * dq2
        den = den * (dq2 * dq2)
        num = jnp.sum(num, axis=1, keepdims=True)
        den = jnp.sum(den, axis=1, keepdims=True)
        sums = jnp.where(lane_s == x - 2, num, sums)
        return jnp.where(lane_s == x + 62, den, sums)

    sums = lax.fori_loop(2, nx + 2, line_plane, jnp.zeros((ny, 128), jnp.float32), unroll=2)

    LS[iz] = sums
    def line_copy(o):
        return pltpu.make_async_remote_copy(
            src_ref=LS.at[iz], dst_ref=LS.at[iz], send_sem=lsend.at[o - 1], recv_sem=lrecv.at[o - 1],
            device_id=(ix, iy, lax.rem(iz + o, NZ)), device_id_type=MESH)
    def line_landing(o):
        src = lax.rem(iz - o + NZ, NZ)
        return pltpu.make_async_remote_copy(
            src_ref=LS.at[src], dst_ref=LS.at[src], send_sem=lsend.at[o - 1], recv_sem=lrecv.at[o - 1],
            device_id=(ix, iy, lax.rem(iz + o, NZ)), device_id_type=MESH)
    for o in range(1, NZ):
        line_copy(o).start()
    for o in range(1, NZ):
        line_landing(o).wait_recv()
    total = LS[0]
    for o in range(1, NZ):
        total = total + LS[o]
    cells = float(nz * NZ)
    line_num = total / cells
    line_den = pltpu.roll(total, 64, 1) / cells
    coef = line_num / (line_den + eps_line)
    masked = jnp.where(lane_s < nx, coef, -jnp.inf)
    here_max = masked[0:8]
    for r in range(8, ny, 8):
        here_max = jnp.maximum(here_max, masked[r : r + 8])
    me = ix * NY + iy
    PS[me] = here_max
    def peak_copy(j, a, b, landing):
        tx, ty = lax.rem(ix + a, NX), lax.rem(iy + b, NY)
        slot = me
        if landing:
            slot = lax.rem(ix - a + NX, NX) * NY + lax.rem(iy - b + NY, NY)
        return pltpu.make_async_remote_copy(
            src_ref=PS.at[slot], dst_ref=PS.at[slot], send_sem=psend.at[j], recv_sem=precv.at[j],
            device_id=(tx, ty, iz), device_id_type=MESH)
    for j, (a, b) in enumerate(plane_peers):
        peak_copy(j, a, b, False).start()
    for o in range(1, NZ):
        line_copy(o).wait_send()
    for j, (a, b) in enumerate(plane_peers):
        peak_copy(j, a, b, True).wait_recv()
    peak = PS[0]
    for j in range(1, NX * NY):
        peak = jnp.maximum(peak, PS[j])
    coef = jnp.minimum(coef, 0.5 * jnp.max(peak, axis=(0, 1), keepdims=True))
    coef_out[...] = coef
    for j, (a, b) in enumerate(plane_peers):
        peak_copy(j, a, b, False).wait_send()
    for n, d in enumerate(offsets):
        def left(n=n, d=d):
            for c in copies(n, d):
                c.wait_send()
        when(exists(d), left)


def scale_kernel(D, coef, visc, coef_out):
    nx, ny = visc.shape[:2]
    lane = lax.broadcasted_iota(jnp.int32, (ny, 128), 1)
    table = coef[...]
    for x in range(nx):
        column = jnp.sum(jnp.where(lane == x, table, 0.0), axis=1, keepdims=True)
        visc[x] = D[x] * column
    coef_out[...] = table.T[0:nx, :]


def per_device(sizes, velocity, metric):
    nx, ny, nz = velocity.shape[1:]
    NX, NY, NZ = sizes
    yr, zr = ny + 8, nz + 128
    packed = -(-12 * nx // 128) * 128
    f32 = jnp.float32
    dmag, coef = pl.pallas_call(
        functools.partial(kernel, sizes),
        out_shape=(jax.ShapeDtypeStruct((nx, ny, nz), f32), jax.ShapeDtypeStruct((ny, 128), f32)),
        in_specs=[pl.BlockSpec(memory_space=pltpu.HBM)] * 2,
        out_specs=(pl.BlockSpec(memory_space=pltpu.VMEM),) * 2,
        scratch_shapes=[
            pltpu.VMEM((6, nx + 4, yr, zr), f32),
            pltpu.VMEM((3, nx + 4, yr, zr), f32),
            pltpu.VMEM((12, nx + 4, ny, nz), f32),
            pltpu.VMEM((3, nx + 4, yr, zr), f32),
            pltpu.VMEM((nx + 4, ny, nz), f32),
            pltpu.VMEM((2, ny, packed), f32),
            pltpu.VMEM((2, 3, 3, ny, packed), f32),
            pltpu.VMEM((NZ, ny, 128), f32),
            pltpu.VMEM((NX * NY, 8, 128), f32),
            pltpu.SemaphoreType.DMA((2,)),
            pltpu.SemaphoreType.DMA((2 * len(offsets),)),
            pltpu.SemaphoreType.DMA((2 * len(offsets),)),
            pltpu.SemaphoreType.DMA((NZ,)),
            pltpu.SemaphoreType.DMA((NZ,)),
            pltpu.SemaphoreType.DMA((NX * NY,)),
            pltpu.SemaphoreType.DMA((NX * NY,)),
        ],
        compiler_params=pltpu.CompilerParams(collective_id=0, has_side_effects=True, vmem_limit_bytes=67043328 - 600 * 1024),
    )(velocity, metric)
    return pl.pallas_call(
        scale_kernel,
        out_shape=(jax.ShapeDtypeStruct((nx, ny, nz), f32), jax.ShapeDtypeStruct((nx, ny), f32)),
        in_specs=[pl.BlockSpec(memory_space=pltpu.VMEM)] * 2,
        out_specs=(pl.BlockSpec(memory_space=pltpu.VMEM),) * 2,
        compiler_params=pltpu.CompilerParams(vmem_limit_bytes=4 * 1024 * 1024),
    )(dmag, coef)


def solution(mesh):
    sizes = (mesh.shape["gx"], mesh.shape["gy"], mesh.shape["gz"])
    return jax.shard_map(
        functools.partial(per_device, sizes),
        mesh=mesh,
        in_specs=(P(None, "gx", "gy", "gz"), P(None, "gx", "gy", "gz")),
        out_specs=(P("gx", "gy", "gz"), P("gx", "gy")),
        check_vma=False,
    )
```

```python
import functools

import jax
import jax.numpy as jnp
from jax import lax
from jax.experimental import pallas as pl
from jax.experimental.pallas import tpu as pltpu
from jax.sharding import PartitionSpec as P

MESH = pl.DeviceIdType.MESH
pairs = ((0, 0), (1, 1), (2, 2), (0, 1), (0, 2), (1, 2))
pair_weight = (1.0, 1.0, 1.0, 2.0, 2.0, 2.0)
eps_line = 1e-06
offsets = [(dx, dy, dz) for dz in (1, -1, 0) for dx in (0, 1, -1) for dy in (0, 1, -1) if (dx, dy, dz) != (0, 0, 0)]


def edge_slots(nx):
    ends = [0, 1, nx - 2, nx - 1]
    order = [(f, x) for f in range(6) for x in ends] + [(f, x) for f in range(6) for x in range(2, nx - 2)]
    return {key: 2 * n for n, key in enumerate(order)}


def kernel(sizes, vel, met, d_out, coef_out, D, V, Gv, G, H, Q, F, PK, R, LS, PS, sem_in, send, recv, lsend, lrecv, psend, precv):
    NX, NY, NZ = sizes
    nx, ny, nz = vel.shape[1:]
    yr, zr = ny + 8, nz + 128
    slots = edge_slots(nx)
    lanes_packed = PK.shape[2]
    ix, iy, iz = lax.axis_index("gx"), lax.axis_index("gy"), lax.axis_index("gz")

    load_v = pltpu.make_async_copy(vel, V.at[0:3, 2 : 2 + nx, 0:ny, 0:nz], sem_in.at[0])
    load_m = pltpu.make_async_copy(met, V.at[3:6, 2 : 2 + nx, 0:ny, 0:nz], sem_in.at[1])
    load_v.start()
    load_m.start()

    def exists(d):
        ok = None
        for delta, i, n in ((d[0], ix, NX), (d[1], iy, NY)):
            if delta:
                c = (i + delta >= 0) & (i + delta < n)
                ok = c if ok is None else ok & c
        return ok

    def when(cond, fn):
        if cond is None:
            fn()
        else:
            pl.when(cond)(fn)

    def dev(d):
        return (ix + d[0], iy + d[1], lax.rem(iz + d[2] + NZ, NZ))

    zplane = jnp.zeros((yr, zr), jnp.float32)
    for f in range(6):
        for xi in (0, 1, nx + 2, nx + 3):
            V[f, xi] = zplane
        def clear(x, _, f=f):
            V[f, x, ny:yr, :] = zplane[0:8]
            return 0
        lax.fori_loop(2, 2 + nx, clear, 0)
    for s in range(2):
        for dx in range(3):
            for dy in range(3):
                R[s, dx, dy] = jnp.zeros((ny, lanes_packed), jnp.float32)

    barrier = pltpu.get_barrier_semaphore()
    expected = jnp.int32(0)
    for d in offsets:
        ok = exists(d)
        def sig(d=d):
            pl.semaphore_signal(barrier, inc=1, device_id=dev(d), device_id_type=MESH)
        when(ok, sig)
        expected = expected + (1 if ok is None else ok.astype(jnp.int32))
    for o in range(1, NZ):
        pl.semaphore_signal(barrier, inc=1, device_id=(ix, iy, lax.rem(iz + o, NZ)), device_id_type=MESH)
    plane_peers = [(a, b) for a in range(NX) for b in range(NY) if (a, b) != (0, 0)]
    for a, b in plane_peers:
        pl.semaphore_signal(barrier, inc=1, device_id=(lax.rem(ix + a, NX), lax.rem(iy + b, NY), iz), device_id_type=MESH)
    expected = expected + (NZ - 1 + len(plane_peers))

    load_v.wait()
    load_m.wait()

    lane = lax.broadcasted_iota(jnp.int32, (ny, 128), 1)
    half = lane // 2
    acc = [[jnp.zeros((ny, 128), jnp.float32) for _ in range(lanes_packed // 128)] for _ in range(2)]
    for (f, x), p in slots.items():
        t, l = divmod(p, 128)
        here = half == l // 2
        hi = V[f, x + 2, 0:ny, nz - 128 : nz]
        lo = V[f, x + 2, 0:ny, 0:128]
        s_hi, s_lo = (l - 126) % 128, l
        acc[0][t] = jnp.where(here, pltpu.roll(hi, s_hi, 1) if s_hi else hi, acc[0][t])
        acc[1][t] = jnp.where(here, pltpu.roll(lo, s_lo, 1) if s_lo else lo, acc[1][t])
    for s in range(2):
        for t in range(lanes_packed // 128):
            PK[s, :, 128 * t : 128 * t + 128] = acc[s][t]

    pl.semaphore_wait(barrier, expected)

    def span_x(dx, metric):
        if dx == 0:
            return (2, 2, nx)
        if dx == 1:
            return (nx + 1, 1, 1) if metric else (nx, 0, 2)
        return (2, nx + 2, 1) if metric else (2, nx + 2, 2)

    def span_y(dy, metric):
        if dy == 0:
            return (0, 0, ny)
        if dy == 1:
            return (ny - 1, ny + 7, 1) if metric else (ny - 2, ny + 6, 2)
        return (0, ny, 1) if metric else (0, ny, 2)

    def copies(n, d):
        dx, dy, dz = d
        out = []
        if dz:
            s = 0 if dz == 1 else 1
            r0, rn = (0, ny) if dy == 0 else ((ny - 8, 8) if dy == 1 else (0, 8))
            ln = lanes_packed if dx == 0 else 128
            out.append((PK.at[s, r0 : r0 + rn, 0:ln], R.at[s, dx + 1, dy + 1, r0 : r0 + rn, 0:ln], 2 * n))
        else:
            for k in range(2):
                xs, xd, xn = span_x(dx, k == 1)
                ys, yd, yn = span_y(dy, k == 1)
                f0 = 3 * k
                out.append((
                    V.at[f0 : f0 + 3, xs : xs + xn, ys : ys + yn, 0:nz],
                    V.at[f0 : f0 + 3, xd : xd + xn, yd : yd + yn, 0:nz],
                    2 * n + k,
                ))
        return [
            pltpu.make_async_remote_copy(src_ref=a, dst_ref=b, send_sem=send.at[j], recv_sem=recv.at[j], device_id=dev(d), device_id_type=MESH)
            for a, b, j in out
        ]

    for n, d in enumerate(offsets):
        def go(n=n, d=d):
            for c in copies(n, d):
                c.start()
        when(exists(d), go)
    def land(wanted):
        for n, d in enumerate(offsets):
            if wanted(d):
                def arrive(n=n, d=d):
                    for c in copies(n, d):
                        c.wait_recv()
                when(exists((-d[0], -d[1], -d[2])), arrive)

    land(lambda d: d[0] == 0 and d[2] != 0)

    lane_r = lax.broadcasted_iota(jnp.int32, (yr, 128), 1)
    low_rows = lax.broadcasted_iota(jnp.int32, (8, 128), 0) < 4
    def packed(s, dx, t):
        cut = slice(128 * t, 128 * t + 128)
        edge = jnp.where(low_rows, R[s, dx, 0, 0:8, cut], R[s, dx, 2, ny - 8 : ny, cut])
        return jnp.concatenate([R[s, dx, 1, :, cut], edge], axis=0)
    tiles = {}
    def fill_span(f, planes):
        for xi in planes:
            if f >= 3 and xi in (0, nx + 3):
                continue
            if xi < 2:
                dx, x = 2, nx - 2 + xi
            elif xi >= nx + 2:
                dx, x = 0, xi - nx - 2
            else:
                dx, x = 1, xi - 2
            t, l = divmod(slots[(f, x)], 128)
            for s in range(2):
                if (s, dx, t) not in tiles:
                    tiles[(s, dx, t)] = packed(s, dx, t)
            a = pltpu.roll(tiles[(0, dx, t)], (126 - l) % 128, 1) if l != 126 else tiles[(0, dx, t)]
            b = pltpu.roll(tiles[(1, dx, t)], (128 - l) % 128, 1) if l else tiles[(1, dx, t)]
            V[f, xi, :, nz:zr] = jnp.where(lane_r < 64, b, a)

    for f in range(6):
        fill_span(f, range(2, nx + 2))
    land(lambda d: d[0] == 0 and d[2] == 0)

    def up(a, axis):
        return pltpu.roll(a, a.shape[axis] - 1, axis)

    def down(a, axis):
        return pltpu.roll(a, 1, axis)

    def smooth(a, axis):
        if axis == 1:
            return (a + a) + (up(a, 1) + down(a, 1))
        t = a + down(a, axis)
        return t + up(t, axis)

    def velocity_plane(x, _):
        for c in range(3):
            Gv[c, x] = smooth(smooth(V[c, x], 0), 1)
        return 0


    def strains(load, m, x):
        d = [[None] * 3 for _ in range(3)]
        for i in range(3):
            here = load(i, x)
            d[i][0] = m[0] * (load(i, x + 1) - load(i, x - 1))
            d[i][1] = m[1] * (up(here, 0) - down(here, 0))
            d[i][2] = m[2] * (up(here, 1) - down(here, 1))
        e = [d[a][b] if a == b else 0.5 * (d[a][b] + d[b][a]) for a, b in pairs]
        square = (e[0] * e[0] + e[1] * e[1] + e[2] * e[2]) + 2.0 * (e[3] * e[3] + e[4] * e[4] + e[5] * e[5])
        return e, jnp.sqrt(0.5 * square)

    def field_plane(x, _):
        m = [V[3 + c, x] for c in range(3)]
        e, mag = strains(lambda i, p: V[i, p], m, x)
        p = m[0][0:ny, 0:nz] * m[1][0:ny, 0:nz] * m[2][0:ny, 0:nz]
        dq = jnp.exp((-2.0 / 3.0) * jnp.log(p))
        Q[x] = dq
        D[jnp.clip(x - 2, 0, nx - 1)] = dq * mag[0:ny, 0:nz]
        for k, (a, b) in enumerate(pairs):
            put(k, x, V[a, x] * V[b, x])
            put(6 + k, x, mag * e[k])
        return 0

    def put(k, x, field):
        for t in range(zr // 128):
            tile = field[:, 128 * t : 128 * t + 128]
            F[k, x, t, 8 : 8 + yr] = tile
            F[k, x, t, 0:8] = tile[ny:yr]

    first = lane == 0
    last = lane == 127

    def smooth_plane(x, _):
        tiles_z = zr // 128
        for k in range(12):
            s = []
            for t in range(tiles_z):
                mid = F[k, x, t, 8 : 8 + ny]
                s.append((F[k, x, t, 7 : 7 + ny] + F[k, x, t, 9 : 9 + ny]) + (mid + mid))
            before = [pltpu.roll(a, 1, 1) for a in s]
            after = [pltpu.roll(a, 127, 1) for a in s]
            for t in range(nz // 128):
                lower = jnp.where(first, before[t - 1], before[t])
                upper = jnp.where(last, after[t + 1], after[t])
                G[k, x, :, 128 * t : 128 * t + 128] = (lower + upper) + (s[t] + s[t])
        return 0

    lax.fori_loop(2, nx + 2, velocity_plane, 0, unroll=8)
    lax.fori_loop(3, nx + 1, field_plane, 0, unroll=2)
    lax.fori_loop(3, nx + 1, smooth_plane, 0, unroll=2)
    land(lambda d: d[0] != 0)
    for f in range(6):
        fill_span(f, (0, 1, nx + 2, nx + 3))
    lax.fori_loop(0, 4, lambda i, c: velocity_plane(jnp.where(i < 2, i, nx + i), c), 0, unroll=4)
    lax.fori_loop(0, 4, lambda i, c: field_plane(jnp.where(i < 2, i + 1, nx + 4 - i), c), 0, unroll=2)
    lax.fori_loop(0, 4, lambda i, c: smooth_plane(jnp.where(i < 2, i + 1, nx + 4 - i), c), 0, unroll=2)

    save = pltpu.make_async_copy(D, d_out, sem_in.at[2])
    save.start()
    row = lax.broadcasted_iota(jnp.int32, (yr, zr), 0)
    has_lo = jnp.where(iy > 0, 1.0, 0.0)
    has_hi = jnp.where(iy < NY - 1, 1.0, 0.0)
    row_scale = jnp.where(row < ny, 1.0, jnp.where(row == ny, has_hi, has_lo)) * (1.0 / 64.0)

    def hat_plane(x, _):
        inside = jnp.where((x == 1) & (ix == 0), 0.0, jnp.where((x == nx + 2) & (ix == NX - 1), 0.0, 1.0))
        for c in range(3):
            mid = Gv[c, x]
            H[c, x] = (Gv[c, x - 1] + Gv[c, x + 1] + (mid + mid)) * (row_scale * inside)
        return 0

    lax.fori_loop(1, nx + 3, hat_plane, 0, unroll=2)

    lane_s = lax.broadcasted_iota(jnp.int32, (ny, 128), 1)

    def line_plane(x, sums):
        d = [[None] * 3 for _ in range(3)]
        hat = []
        for i in range(3):
            here = H[i, x]
            core = here[0:ny]
            hat.append(core[:, 0:nz])
            d[i][0] = V[3, x, 0:ny, 0:nz] * (H[i, x + 1, 0:ny, 0:nz] - H[i, x - 1, 0:ny, 0:nz])
            d[i][1] = V[4, x, 0:ny, 0:nz] * (up(here, 0) - down(here, 0))[0:ny, 0:nz]
            d[i][2] = V[5, x, 0:ny, 0:nz] * (up(core, 1) - down(core, 1))[:, 0:nz]
        e = [d[a][b] if a == b else 0.5 * (d[a][b] + d[b][a]) for a, b in pairs]
        square = (e[0] * e[0] + e[1] * e[1] + e[2] * e[2]) + 2.0 * (e[3] * e[3] + e[4] * e[4] + e[5] * e[5])
        mag2 = 2.0 * jnp.sqrt(0.5 * square)
        num = den = 0.0
        for k, (a, b) in enumerate(pairs):
            vv, ms = G[k, x], G[6 + k, x]
            vv = (G[k, x - 1] + G[k, x + 1] + (vv + vv)) * (1.0 / 64.0)
            ms = (G[6 + k, x - 1] + G[6 + k, x + 1] + (ms + ms)) * (1.0 / 128.0)
            leonard = vv - hat[a] * hat[b]
            model = ms - mag2 * e[k]
            n, m2 = leonard * model, model * model
            if pair_weight[k] != 1.0:
                n, m2 = pair_weight[k] * n, pair_weight[k] * m2
            num, den = num + n, den + m2
        dq2 = 2.0 * Q[x]
        num = num * dq2
        den = den * (dq2 * dq2)
        num = jnp.sum(num, axis=1, keepdims=True)
        den = jnp.sum(den, axis=1, keepdims=True)
        sums = jnp.where(lane_s == x - 2, num, sums)
        return jnp.where(lane_s == x + 62, den, sums)

    sums = lax.fori_loop(2, nx + 2, line_plane, jnp.zeros((ny, 128), jnp.float32), unroll=8)

    LS[iz] = sums
    def line_copy(o):
        return pltpu.make_async_remote_copy(
            src_ref=LS.at[iz], dst_ref=LS.at[iz], send_sem=lsend.at[o - 1], recv_sem=lrecv.at[o - 1],
            device_id=(ix, iy, lax.rem(iz + o, NZ)), device_id_type=MESH)
    def line_landing(o):
        src = lax.rem(iz - o + NZ, NZ)
        return pltpu.make_async_remote_copy(
            src_ref=LS.at[src], dst_ref=LS.at[src], send_sem=lsend.at[o - 1], recv_sem=lrecv.at[o - 1],
            device_id=(ix, iy, lax.rem(iz + o, NZ)), device_id_type=MESH)
    for o in range(1, NZ):
        line_copy(o).start()
    for o in range(1, NZ):
        line_landing(o).wait_recv()
    total = LS[0]
    for o in range(1, NZ):
        total = total + LS[o]
    cells = float(nz * NZ)
    line_num = total / cells
    line_den = pltpu.roll(total, 64, 1) / cells
    coef = line_num / (line_den + eps_line)
    masked = jnp.where(lane_s < nx, coef, -jnp.inf)
    here_max = masked[0:8]
    for r in range(8, ny, 8):
        here_max = jnp.maximum(here_max, masked[r : r + 8])
    me = ix * NY + iy
    PS[me] = here_max
    def peak_copy(j, a, b, landing):
        tx, ty = lax.rem(ix + a, NX), lax.rem(iy + b, NY)
        slot = me
        if landing:
            slot = lax.rem(ix - a + NX, NX) * NY + lax.rem(iy - b + NY, NY)
        return pltpu.make_async_remote_copy(
            src_ref=PS.at[slot], dst_ref=PS.at[slot], send_sem=psend.at[j], recv_sem=precv.at[j],
            device_id=(tx, ty, iz), device_id_type=MESH)
    for j, (a, b) in enumerate(plane_peers):
        peak_copy(j, a, b, False).start()
    for o in range(1, NZ):
        line_copy(o).wait_send()
    for j, (a, b) in enumerate(plane_peers):
        peak_copy(j, a, b, True).wait_recv()
    peak = PS[0]
    for j in range(1, NX * NY):
        peak = jnp.maximum(peak, PS[j])
    coef = jnp.minimum(coef, 0.5 * jnp.max(peak, axis=(0, 1), keepdims=True))
    coef_out[...] = coef
    save.wait()
    for j, (a, b) in enumerate(plane_peers):
        peak_copy(j, a, b, False).wait_send()
    for n, d in enumerate(offsets):
        def left(n=n, d=d):
            for c in copies(n, d):
                c.wait_send()
        when(exists(d), left)


def scale_kernel(D, coef, visc, coef_out):
    nx, ny = visc.shape[:2]
    lane = lax.broadcasted_iota(jnp.int32, (ny, 128), 1)
    table = coef[...]
    for x in range(nx):
        column = jnp.sum(jnp.where(lane == x, table, 0.0), axis=1, keepdims=True)
        visc[x] = D[x] * column
    coef_out[...] = table.T[0:nx, :]


def per_device(sizes, velocity, metric):
    nx, ny, nz = velocity.shape[1:]
    NX, NY, NZ = sizes
    yr, zr = ny + 8, nz + 128
    packed = -(-12 * nx // 128) * 128
    f32 = jnp.float32
    dmag, coef = pl.pallas_call(
        functools.partial(kernel, sizes),
        out_shape=(jax.ShapeDtypeStruct((nx, ny, nz), f32), jax.ShapeDtypeStruct((ny, 128), f32)),
        in_specs=[pl.BlockSpec(memory_space=pltpu.HBM)] * 2,
        out_specs=(pl.BlockSpec(memory_space=pltpu.HBM), pl.BlockSpec(memory_space=pltpu.VMEM)),
        scratch_shapes=[
            pltpu.VMEM((nx, ny, nz), f32),
            pltpu.VMEM((6, nx + 4, yr, zr), f32),
            pltpu.VMEM((3, nx + 4, yr, zr), f32),
            pltpu.VMEM((12, nx + 4, ny, nz), f32),
            pltpu.VMEM((3, nx + 4, yr, zr), f32),
            pltpu.VMEM((nx + 4, ny, nz), f32),
            pltpu.VMEM((12, nx + 4, zr // 128, 8 + yr, 128), f32),
            pltpu.VMEM((2, ny, packed), f32),
            pltpu.VMEM((2, 3, 3, ny, packed), f32),
            pltpu.VMEM((NZ, ny, 128), f32),
            pltpu.VMEM((NX * NY, 8, 128), f32),
            pltpu.SemaphoreType.DMA((3,)),
            pltpu.SemaphoreType.DMA((2 * len(offsets),)),
            pltpu.SemaphoreType.DMA((2 * len(offsets),)),
            pltpu.SemaphoreType.DMA((NZ,)),
            pltpu.SemaphoreType.DMA((NZ,)),
            pltpu.SemaphoreType.DMA((NX * NY,)),
            pltpu.SemaphoreType.DMA((NX * NY,)),
        ],
        compiler_params=pltpu.CompilerParams(collective_id=0, has_side_effects=True, vmem_limit_bytes=67043328 - 600 * 1024),
    )(velocity, metric)
    return pl.pallas_call(
        scale_kernel,
        out_shape=(jax.ShapeDtypeStruct((nx, ny, nz), f32), jax.ShapeDtypeStruct((nx, ny), f32)),
        in_specs=[pl.BlockSpec(memory_space=pltpu.VMEM)] * 2,
        out_specs=(pl.BlockSpec(memory_space=pltpu.VMEM),) * 2,
        compiler_params=pltpu.CompilerParams(vmem_limit_bytes=4 * 1024 * 1024),
    )(dmag, coef)


def solution(mesh):
    sizes = (mesh.shape["gx"], mesh.shape["gy"], mesh.shape["gz"])
    return jax.shard_map(
        functools.partial(per_device, sizes),
        mesh=mesh,
        in_specs=(P(None, "gx", "gy", "gz"), P(None, "gx", "gy", "gz")),
        out_specs=(P("gx", "gy", "gz"), P("gx", "gy")),
        check_vma=False,
    )
```
